32 devices in a mesh: grp: 2 (over x), grid: 16 (over z, y, core).
Axes of the slice: x: 2, y: 2, z: 4, core: 2. Of those that a mesh axis runs over, the one named last changes fastest.
Arguments:
- valence: bfloat16 [32768, 48], P(('grp', 'grid')), parts along dimension 0, may hold values from -24 to 24
- conduction: bfloat16 [32768, 512], P(('grp', 'grid')), parts along dimension 0, may hold values from -6 to 6
- potentials: bfloat16 [32768, 64], P(('grp', 'grid')), parts along dimension 0, may hold values from -6 to 6
- eigenpotentials: bfloat16 [32768, 1024], P(('grp', 'grid')), parts along dimension 0, may hold values from -0.1875 to 0.1875
- valence_energy: float32 [96], P('grp'), parts along dimension 0, may hold values from -6 to -1
- conduction_energy: float32 [1024], P('grp'), parts along dimension 0, may hold values from 0.5 to 20
Outputs:
- projected: float32 [2048, 64], P(('grp', 'grid')), parts along dimension 0
- complementary: float32 [32768, 64], P(('grp', 'grid')), parts along dimension 0
The draws below stay inside these ranges and needn't reach their ends.
There are 2 independent parts, one for each index of `grp`. The reference program is written for one: setup_inputs(seed, part) draws one part's arguments, and reference() takes and returns one part's arrays. A program takes and returns all parts, laid end to end along the dimension named above; each array names one. Nothing has to cross between parts.
All inputs are finite; a program needn't handle non-finite values.
Results may differ from the reference program's by a relative error of at most 0.0042.
Values may be sent and summed in bfloat16 or wider, within the bound.
No kernel may reach another device: no remote copies, remote signals or barrier semaphores. Data moves between devices by JAX's collectives and lax.ppermute only.
A program may use at most 64 MiB of HBM per device.

```python
import math
import jax
import jax.numpy as jnp
from jax import lax

NV = 48
NC = 512
NP = 64
NE = 1024
POINTS = 16384


def draw_valence(key, part):
    key_list = jax.random.split(key, 3)
    position = jnp.arange(POINTS, dtype=jnp.float32) / (POINTS - 1)
    envelope = jnp.sqrt(1.0 + 2.0 * position)
    values = jnp.clip(jax.random.normal(key_list[0], (POINTS, NV), jnp.float32), -4.0, 4.0)
    spread = 10.0 ** jax.random.uniform(key_list[2], (POINTS, 1), jnp.float32, -0.5, 0.5)
    return jnp.clip(values * envelope[:, None] * spread, -24.0, 24.0).astype(jnp.bfloat16)


def draw_eigenpotentials(key, part):
    key_list = jax.random.split(key, 2)
    column = jnp.arange(NE, dtype=jnp.float32) / (NE - 1)
    spread = 10.0 ** jax.random.uniform(key_list[1], (1, NE), jnp.float32, -0.5, 0.5)
    envelope = jnp.sqrt(1.0 + 2.0 * column)
    values = jnp.clip(jax.random.normal(key_list[0], (POINTS, NE), jnp.float32), -4.0, 4.0)
    factor = POINTS ** (-0.5)
    return jnp.clip(values * envelope[None, :] * spread * factor, -24.0 * factor, 24.0 * factor).astype(jnp.bfloat16)


def steps_of(rng, extent, shards, low, largest):
    level = 1.0
    for dim, parts in shards:
        steps = jax.random.uniform(jax.random.fold_in(jax.random.fold_in(rng, 6), dim), (parts,), jnp.float32, low / len(shards), largest / len(shards))
        level = level * jnp.repeat(jnp.exp(steps), extent[dim] // parts).reshape((-1,) + (1,) * (len(extent) - 1 - dim))
    return level


def noise(own_key, shape, width, reach, cuts=(), held_as=jnp.bfloat16):
    level = steps_of(own_key, shape, cuts, -0.22, 0.18) if cuts else 1.0
    result = jax.random.normal(own_key, shape, jnp.float32) * width * level
    return jnp.minimum(jnp.maximum(result, -reach), reach).astype(held_as)


def setup_inputs(seed: int = 0, part: int = 0) -> dict:
    arg_keys = jax.random.split(jax.random.key(seed), 7)
    part_keys = jax.random.split(jax.random.fold_in(arg_keys[6], part), 7)
    return {
        "valence": draw_valence(jax.random.fold_in(jax.random.fold_in(arg_keys[6], part), 71), part),
        "conduction": noise(part_keys[1], (POINTS, NC), 1.0, 6.0, ((0, 16),)),
        "potentials": noise(part_keys[2], (POINTS, NP), 1.0, 6.0, ((0, 16),)),
        "eigenpotentials": draw_eigenpotentials(jax.random.fold_in(jax.random.fold_in(arg_keys[6], part), 71), part),
        "valence_energy": jnp.clip(jax.random.uniform(part_keys[4], (NV,), jnp.float32, -6.0, -1.0), -6.0, -1.0),
        "conduction_energy": jnp.clip(jnp.exp(jax.random.uniform(part_keys[5], (NC,), jnp.float32, math.log(0.5), math.log(20.0))), 0.5, 20.0),
    }


def pair_products(val_block, pot_block):
    joined = pot_block.astype(jnp.float32)[:, :, None] * val_block.astype(jnp.float32)[:, None, :]
    return joined.reshape(val_block.shape[0], -1).astype(jnp.bfloat16)

def reference(valence, conduction, potentials, eigenpotentials, valence_energy, conduction_energy):
    points_total = valence.shape[0]
    valence_count = valence.shape[1]
    conduction_count = conduction.shape[1]
    potential_count = potentials.shape[1]
    block_size = min(4096, points_total)
    block_count = points_total // block_size
    val_blocks = valence.reshape(block_count, block_size, valence_count)
    cond_blocks = conduction.reshape(block_count, block_size, conduction_count)
    pot_blocks = potentials.reshape(block_count, block_size, potential_count)

    def add_block(carried, blocks_in):
        val_block, cond_block, pot_block = blocks_in
        paired = pair_products(val_block, pot_block)
        return (carried + lax.dot_general(cond_block, paired, (((0,), (0,)), ((), ())), preferred_element_type=jnp.float32), None)
    initial = jnp.zeros((conduction_count, potential_count * valence_count), jnp.float32)
    coefficients, _ = lax.scan(add_block, initial, (val_blocks, cond_blocks, pot_blocks))
    denominators = valence_energy[None, :] - conduction_energy[:, None]
    scaled = (coefficients.reshape(conduction_count, potential_count, valence_count) * (4.0 / points_total) / denominators[:, None, :]).reshape(conduction_count, potential_count * valence_count).astype(jnp.bfloat16)

    def respond(blocks_in):
        val_block, cond_block = blocks_in
        combined = jnp.dot(cond_block, scaled, preferred_element_type=jnp.float32)
        return lax.optimization_barrier(jnp.sum(combined.reshape(block_size, potential_count, valence_count) * val_block.astype(jnp.float32)[:, None, :], axis=2))
    response = lax.map(respond, (val_blocks, cond_blocks)).reshape(points_total, potential_count)
    response_low = response.astype(jnp.bfloat16)
    intersection = lax.dot_general(eigenpotentials, response_low, (((0,), (0,)), ((), ())), preferred_element_type=jnp.float32)
    projected = intersection / jnp.sqrt(lax.optimization_barrier(jnp.mean(intersection * intersection, axis=0)) + 1e-06)
    intersection_low = intersection.astype(jnp.bfloat16)
    remainder = response - jnp.dot(eigenpotentials, intersection_low, preferred_element_type=jnp.float32)
    complementary = remainder / jnp.sqrt(lax.optimization_barrier(jnp.mean(remainder * remainder, axis=0)) + 1e-06)
    return (projected, complementary)
```

```python
import jax
import jax.numpy as jnp
from jax import lax
from jax.sharding import PartitionSpec as P

F32 = jnp.float32
BF16 = jnp.bfloat16
CHUNKS = 2


def swap(block, bit):
    count = lax.axis_size("grid")
    return lax.ppermute(block, "grid", [(i, i ^ bit) for i in range(count)])


def pairs_of(pot_rows, val_rows):
    joined = pot_rows.astype(F32)[:, None, :] * val_rows.astype(F32)[None, :, :]
    return joined.reshape(-1, joined.shape[2]).astype(BF16)


def contract(left, right):
    return jnp.dot(left, right, preferred_element_type=F32)


def body(valence, conduction, potentials, eigenpotentials, valence_energy, conduction_energy):
    rows, val_count = valence.shape
    cond_count = conduction.shape[1]
    pot_count = potentials.shape[1]
    eig_count = eigenpotentials.shape[1]
    count = lax.axis_size("grid")
    points_total = rows * count
    me = lax.axis_index("grid")
    core = me & 1
    side = (me >> 1) & 1
    bits = []
    bit = 4
    while bit < count:
        bits.append(bit)
        bit *= 2
    spread, last = bits[:-1], bits[-1]
    k_half, c_half = pot_count // 2, cond_count // 2
    c_part = c_half // CHUNKS

    small = jnp.concatenate([valence, potentials], axis=1).T
    def c_block(which, part):
        return lax.dynamic_slice(conduction, (0, which * c_half + part * c_part), (rows, c_part))
    small_side = swap(small, 2)
    cond_side = [swap(c_block(1 - side, part), 2) for part in range(CHUNKS)]
    small_core = swap(small, 1)
    cond_core = [swap(c_block(side, part), 1) for part in range(CHUNKS)]
    small_diag = swap(small_side, 1)
    cond_diag = [swap(block, 1) for block in cond_side]
    eig_core = swap(eigenpotentials, 1)
    cond_here = [jnp.concatenate([c_block(side, part), cond_core[part]], axis=0) for part in range(CHUNKS)]
    cond_there = [jnp.concatenate([cond_side[part], cond_diag[part]], axis=0) for part in range(CHUNKS)]
    small_here = jnp.concatenate([small, small_core], axis=1)
    small_there = jnp.concatenate([small_side, small_diag], axis=1)
    val_here, val_there = small_here[:val_count], small_there[:val_count]
    def pots(block, first, size):
        return lax.dynamic_slice(block, (val_count + first, 0), (size, block.shape[1]))

    energies = lax.dynamic_slice(conduction_energy, (side * c_half,), (c_half,))
    denominators = valence_energy[:, None] - energies[None, :]

    first, size = core * k_half, k_half
    groups = []
    for bit in spread:
        size //= 2
        up = (me & bit) // bit
        groups.append((first + (1 - up) * size, size))
        first = first + up * size
    groups.append((first, size))
    def coefficients(group, part):
        start, many = group
        return contract(pairs_of(pots(small_here, start, many), val_here), cond_here[part]) + contract(
            pairs_of(pots(small_there, start, many), val_there), cond_there[part]
        )
    scaled_parts = []
    for part in range(CHUNKS):
        total = None
        for level, bit in enumerate(spread):
            mine = coefficients(groups[level], part)
            up, many = (me & bit) // bit, mine.shape[0]
            if total is not None:
                mine = mine + lax.dynamic_slice(total, ((1 - up) * many, 0), mine.shape)
                total = lax.dynamic_slice(total, (up * many, 0), mine.shape)
            got = swap(mine.astype(BF16), bit).astype(F32)
            total = got if total is None else total + got
        mine = coefficients(groups[-1], part)
        total = mine if total is None else mine + total
        total = total + swap(total.astype(BF16), last).astype(F32)
        den = denominators[:, part * c_part : (part + 1) * c_part]
        shaped = total.reshape(size, val_count, c_part)
        scaled = ((shaped * (4.0 / points_total)) / den[None]).astype(BF16).reshape(size * val_count, c_part)
        for bit in reversed(spread):
            scaled = jnp.concatenate([scaled, swap(scaled, bit)], axis=0)
        scaled_parts.append(scaled)
    scaled = jnp.concatenate(scaled_parts, axis=1)

    def respond(cond_parts, val_block):
        cond_block = jnp.concatenate(cond_parts, axis=1)
        combined = lax.dot_general(scaled, cond_block, (((1,), (1,)), ((), ())), preferred_element_type=F32)
        combined = combined.reshape(k_half, val_count, cond_block.shape[0])
        return jnp.sum(combined * val_block.astype(F32)[None], axis=1)
    response_there = respond(cond_there, val_there)
    arrived = swap(response_there, 2)
    response = respond(cond_here, val_here) + arrived
    shape = response.shape
    for level, bit in enumerate(spread):
        shaped = response.reshape((1 << level, 2, shape[0] // (2 << level)) + shape[1:])
        up = (me & bit) != 0
        response = jnp.where(up, shaped[:, ::-1], shaped).reshape(shape)

    eig_here = jnp.concatenate([eigenpotentials, eig_core], axis=0)
    intersection = contract(response.astype(BF16), eig_here)
    for bit in [2] + bits:
        intersection = intersection + swap(intersection, bit)
    squares = jnp.mean(intersection * intersection, axis=1, keepdims=True)
    unit = intersection / jnp.sqrt(squares + 1e-06)
    eig_rows = eig_count // count
    def e_block(device):
        return lax.dynamic_slice(unit, (0, device * eig_rows), (k_half, eig_rows))
    mine, other = e_block(me), swap(e_block(me ^ 1), 1)
    def joined(mine, other):
        return jnp.where(core == 0, jnp.concatenate([mine, other], 0), jnp.concatenate([other, mine], 0))
    projected = joined(mine, other).T

    back = lax.dot_general(intersection.astype(BF16), eig_here, (((1,), (1,)), ((), ())), preferred_element_type=F32)
    remainder = response - back
    remainder_other = swap(remainder[:, rows:], 1)
    total = jnp.broadcast_to(jnp.sum(remainder * remainder, axis=1)[None, :], (8, k_half))
    for bit in [2] + bits:
        total = total + swap(total, bit)
    total_other = swap(total, 1)
    sums = joined(total[0], total_other[0])
    complementary = joined(remainder[:, :rows], remainder_other).T / jnp.sqrt(sums / points_total + 1e-06)[None, :]
    return (projected, complementary)


def solution(mesh):
    spec = P(("grp", "grid"), None)
    return jax.shard_map(
        body,
        mesh=mesh,
        in_specs=(spec, spec, spec, spec, P("grp"), P("grp")),
        out_specs=(spec, spec),
        check_vma=False,
    )
```

```python
import functools

import jax
import jax.numpy as jnp
from jax import lax
from jax.experimental import pallas as pl
from jax.experimental.pallas import tpu as pltpu

from jax.sharding import PartitionSpec as P

F32 = jnp.float32
BF16 = jnp.bfloat16
CHUNKS = 2
PIECES = 1


def swap(block, bit):
    count = lax.axis_size("grid")
    return lax.ppermute(block, "grid", [(i, i ^ bit) for i in range(count)])


def pairs_of(pot_rows, val_rows):
    joined = pot_rows[:, None, :] * val_rows[None, :, :]
    return joined.reshape(-1, joined.shape[2])


def contract(left, right):
    return jnp.dot(left, right, preferred_element_type=F32)


def contract_last(left, right):
    return lax.dot_general(left, right, (((1,), (1,)), ((), ())), preferred_element_type=F32)


def body(valence, conduction, potentials, eigenpotentials, valence_energy, conduction_energy):
    rows, val_count = valence.shape
    cond_count = conduction.shape[1]
    pot_count = potentials.shape[1]
    eig_count = eigenpotentials.shape[1]
    count = lax.axis_size("grid")
    points_total = rows * count
    me = lax.axis_index("grid")
    core = me & 1
    side = (me >> 1) & 1
    bits = []
    bit = 4
    while bit < count:
        bits.append(bit)
        bit *= 2
    spread, last = bits[:-1], bits[-1]
    k_half, c_half = pot_count // 2, cond_count // 2
    c_part = c_half // CHUNKS
    parts = range(CHUNKS)

    blocks = pl.pallas_call(
        functools.partial(prepare_kernel, CHUNKS),
        out_shape=[jax.ShapeDtypeStruct((rows, c_part), BF16)] * (2 * CHUNKS),
        in_specs=[pl.BlockSpec(memory_space=pltpu.SMEM), pl.BlockSpec(memory_space=pltpu.VMEM)],
        out_specs=[pl.BlockSpec(memory_space=pltpu.VMEM)] * (2 * CHUNKS),
        compiler_params=pltpu.CompilerParams(vmem_limit_bytes=6 * 2**20),
        cost_estimate=pl.CostEstimate(flops=10**6, bytes_accessed=2**21, transcendentals=0),
    )(side[None], conduction)
    vals, pots = [valence.T], [potentials.T]
    val_side, pot_side = swap(vals[0], 2), swap(pots[0], 2)
    cond_side = [swap(blocks[part], 2) for part in parts]
    cond_mine = blocks[CHUNKS:]
    vals += [swap(vals[0], 1), val_side, swap(val_side, 1)]
    pots += [swap(pots[0], 1), pot_side, swap(pot_side, 1)]
    cond_core = [swap(cond_mine[part], 1) for part in parts]
    cond_diag = [swap(cond_side[part], 1) for part in parts]
    eig_core = swap(eigenpotentials, 1)
    cond_all = [cond_mine, cond_core, cond_side, cond_diag]

    energies = lax.dynamic_slice(conduction_energy, (side * c_half,), (c_half,))
    factors = (4.0 / points_total) / (valence_energy[:, None] - energies[None, :])

    first, size = core * k_half, k_half
    groups = []
    for bit in spread:
        size //= 2
        up = (me & bit) // bit
        groups.append((first + (1 - up) * size, size))
        first = first + up * size
    groups.append((first, size))

    def pairs_for(place, group):
        block = pots[place]
        return pairs_of(lax.dynamic_slice(block, (group[0], 0), (group[1], block.shape[1])), vals[place])

    starts = jnp.stack([group[0] for group in groups])
    own = [cond_all[place][part] for place in (0, 1) for part in parts]
    own_terms = pl.pallas_call(
        functools.partial(own_kernel, CHUNKS),
        out_shape=[
            jax.ShapeDtypeStruct((group[1] * val_count, c_part), F32) for group in groups for part in parts
        ],
        in_specs=[pl.BlockSpec(memory_space=pltpu.SMEM)] + [pl.BlockSpec(memory_space=pltpu.VMEM)] * (4 + len(own)),
        out_specs=[pl.BlockSpec(memory_space=pltpu.VMEM)] * (len(groups) * CHUNKS),
        scratch_shapes=[
            pltpu.VMEM((groups[0][1] * val_count, 2 * rows), BF16),
            pltpu.VMEM((2 * rows, c_half), BF16),
            pltpu.VMEM((2, pot_count, rows), F32),
        ],
        compiler_params=pltpu.CompilerParams(vmem_limit_bytes=16 * 2**20),
        cost_estimate=pl.CostEstimate(
            flops=4 * rows * k_half * val_count * c_half, bytes_accessed=2**22, transcendentals=0
        ),
    )(starts, vals[0], vals[1], pots[0], pots[1], *own)
    pairs = {place: [pairs_for(place, group) for group in groups] for place in (2, 3)}

    def coefficients(index, part):
        total = own_terms[index * CHUNKS + part]
        for place in (2, 3):
            total = total + contract(pairs[place][index], cond_all[place][part])
        return total

    def cut(block):
        return jnp.split(block, PIECES, axis=0)

    scaled_mine, scaled_rest = [], []
    for part in parts:
        totals = [None] * PIECES
        for level, bit in enumerate(spread):
            mine = cut(coefficients(level, part))
            up = (me & bit) // bit
            for q in range(PIECES):
                send, many = mine[q], mine[q].shape[0]
                if totals[q] is not None:
                    send = send + lax.dynamic_slice(totals[q], ((1 - up) * many, 0), send.shape)
                    totals[q] = lax.dynamic_slice(totals[q], (up * many, 0), send.shape)
                got = swap(send.astype(BF16), bit).astype(F32)
                totals[q] = got if totals[q] is None else totals[q] + got
        mine = cut(coefficients(len(spread), part))
        factor = factors[:, part * c_part : (part + 1) * c_part]
        own, rest = [], []
        for q in range(PIECES):
            total = mine[q] if totals[q] is None else mine[q] + totals[q]
            total = total + swap(total.astype(BF16), last).astype(F32)
            many = total.shape[0] // val_count
            shaped = total.reshape(many, val_count, c_part)
            scaled = (shaped * factor[None]).astype(BF16).reshape(total.shape)
            own.append(scaled)
            others = []
            for level in reversed(range(len(spread))):
                known = jnp.concatenate([scaled] + others, axis=0)
                others.append(swap(known, spread[level]))
            if others:
                rest.append(jnp.concatenate(others, axis=0))
        scaled_mine.append(own)
        scaled_rest.append(rest)
    many = k_half // PIECES >> len(spread)

    def respond(blocks, places):
        kernel = functools.partial(respond_kernel, len(places), CHUNKS, len(blocks[0]))
        operands = [block for column in blocks for block in column]
        operands += [cond_all[place][part] for place in places for part in parts]
        operands += [vals[place] for place in places]
        height = sum(block.shape[0] for block in blocks[0])
        return pl.pallas_call(
            kernel,
            out_shape=jax.ShapeDtypeStruct((height // val_count, rows * len(places)), F32),
            in_specs=[pl.BlockSpec(memory_space=pltpu.VMEM)] * len(operands),
            out_specs=pl.BlockSpec(memory_space=pltpu.VMEM),
            scratch_shapes=[pltpu.VMEM((height, c_half), BF16)],
            compiler_params=pltpu.CompilerParams(vmem_limit_bytes=8 * 2**20),
            cost_estimate=pl.CostEstimate(
                flops=2 * height * c_half * rows * len(places), bytes_accessed=2**22, transcendentals=0
            ),
        )(*operands)

    here, there = (0, 1), (2, 3)
    kinds = [scaled_mine] + ([scaled_rest] if spread else [])
    sums = []
    for blocks in kinds:
        arrived = swap(respond(blocks, there), 2)
        sums.append(respond(blocks, here) + arrived)
    width = sums[0].shape[1]
    ordered = [block.reshape(PIECES, -1, many, width) for block in sums]
    response = jnp.concatenate(ordered, axis=1).swapaxes(0, 1).reshape(k_half, width)
    for level, bit in enumerate(spread):
        shaped = response.reshape(1 << level, 2, -1, width)
        response = jnp.where((me & bit) != 0, shaped[:, ::-1], shaped).reshape(k_half, width)

    low = response.astype(BF16)
    intersection = contract(low[:, :rows], eigenpotentials) + contract(low[:, rows:], eig_core)
    for bit in [2] + spread:
        intersection = intersection + swap(intersection, bit)
    intersection = intersection + swap(intersection.astype(BF16), last).astype(F32)
    squares = jnp.mean(intersection * intersection, axis=1, keepdims=True)
    unit = intersection / jnp.sqrt(squares + 1e-06)
    eig_rows = eig_count // count

    def e_block(device):
        return lax.dynamic_slice(unit, (0, device * eig_rows), (k_half, eig_rows))

    def joined(mine, other):
        return jnp.where(core == 0, jnp.concatenate([mine, other], 0), jnp.concatenate([other, mine], 0))

    projected = joined(e_block(me), swap(e_block(me ^ 1), 1)).T

    ilow = intersection.astype(BF16)
    remainder_core = response[:, rows:] - contract_last(ilow, eig_core)
    remainder_mine = response[:, :rows] - contract_last(ilow, eigenpotentials)
    remainder_other = swap(remainder_core, 1)
    share = jnp.sum(remainder_core * remainder_core, axis=1) + jnp.sum(remainder_mine * remainder_mine, axis=1)
    share = share[None, :]
    for low_bit, high_bit in zip(bits[::2], bits[1::2] + [0] * (len(bits) % 2)):
        steps = [step for step in (low_bit, high_bit, low_bit | high_bit) if step and (high_bit or step == low_bit)]
        share = share + sum(swap(share, step) for step in dict.fromkeys(steps))
    mine, other = share + swap(share, 2), swap(share, 1) + swap(share, 3)
    sums = joined(mine, other).reshape(pot_count)
    scale = jnp.sqrt(sums / points_total + 1e-06)
    turned = lax.optimization_barrier(joined(remainder_mine, remainder_other).T)
    return (projected, turned / scale[None, :])


def prepare_kernel(chunks, side_ref, cond_ref, *blocks):
    width = blocks[0].shape[1]
    side = side_ref[0]
    for index, block in enumerate(blocks):
        which = 1 - side if index < chunks else side
        begin = pl.multiple_of((which * chunks + index % chunks) * width, width)
        block[...] = cond_ref[:, pl.ds(begin, width)]


def own_kernel(chunks, starts_ref, val0, val1, pot0, pot1, *refs):
    conds, outs = refs[: 2 * chunks], refs[2 * chunks : -3]
    pairs, right, wide = refs[-3:]
    val_count, rows = val0.shape
    width = conds[0].shape[1]
    for place, (val, pot) in enumerate(((val0, pot0), (val1, pot1))):
        for part in range(chunks):
            right[pl.ds(place * rows, rows), pl.ds(part * width, width)] = conds[place * chunks + part][...]
        wide[place] = pot[...].astype(F32)
    for group in range(len(outs) // chunks):
        height = outs[group * chunks].shape[0]
        many = height // val_count
        start = starts_ref[group]
        for place, val in enumerate((val0, val1)):
            values = val[...].astype(F32)
            for k in range(many):
                row = wide[place, pl.ds(start + k, 1), :]
                pairs[pl.ds(k * val_count, val_count), pl.ds(place * rows, rows)] = (row * values).astype(BF16)
        total = contract(pairs[pl.ds(0, height), :], right[...])
        for part in range(chunks):
            outs[group * chunks + part][...] = total[:, part * width : (part + 1) * width]


def respond_kernel(places, chunks, pieces, *refs):
    scaled = refs[: chunks * pieces]
    conds = refs[chunks * pieces :][: places * chunks]
    vals = refs[chunks * pieces + places * chunks :][:places]
    out, left = refs[-2:]
    height, depth = left.shape
    width = depth // chunks
    for part in range(chunks):
        top = 0
        for q in range(pieces):
            block = scaled[part * pieces + q]
            left[pl.ds(top, block.shape[0]), pl.ds(part * width, width)] = block[...]
            top += block.shape[0]
    count = out.shape[0]
    val_count = height // count
    rows = out.shape[1] // places
    tile = min(rows, 256)
    for place in range(places):

        def step(index, carry):
            begin = pl.multiple_of(index * tile, tile)
            right = jnp.concatenate(
                [conds[place * chunks + part][pl.ds(begin, tile), :] for part in range(chunks)], axis=1
            )
            values = vals[place][:, pl.ds(begin, tile)].astype(F32)
            product = contract_last(left[...], right)
            summed = jnp.sum(product.reshape(count, val_count, tile) * values[None], axis=1)
            out[:, pl.ds(pl.multiple_of(place * rows + begin, tile), tile)] = summed
            return carry

        lax.fori_loop(0, rows // tile, step, 0)


def solution(mesh):
    spec = P(("grp", "grid"), None)

    return jax.shard_map(
        body,
        mesh=mesh,
        in_specs=(spec, spec, spec, spec, P("grp"), P("grp")),
        out_specs=(spec, spec),
        check_vma=False,
    )
```

```python
import functools

import jax
import jax.numpy as jnp
from jax import lax
from jax.experimental import pallas as pl
from jax.experimental.pallas import tpu as pltpu

from jax.sharding import PartitionSpec as P

F32 = jnp.float32
BF16 = jnp.bfloat16
CHUNKS = 2
PIECES = 2


def swap(block, bit):
    count = lax.axis_size("grid")
    return lax.ppermute(block, "grid", [(i, i ^ bit) for i in range(count)])


def pairs_of(pot_rows, val_rows):
    joined = pot_rows[:, None, :] * val_rows[None, :, :]
    return joined.reshape(-1, joined.shape[2])


def contract(left, right):
    return jnp.dot(left, right, preferred_element_type=F32)


def contract_last(left, right):
    return lax.dot_general(left, right, (((1,), (1,)), ((), ())), preferred_element_type=F32)


def body(valence, conduction, potentials, eigenpotentials, valence_energy, conduction_energy):
    rows, val_count = valence.shape
    cond_count = conduction.shape[1]
    pot_count = potentials.shape[1]
    eig_count = eigenpotentials.shape[1]
    count = lax.axis_size("grid")
    points_total = rows * count
    me = lax.axis_index("grid")
    core = me & 1
    side = (me >> 1) & 1
    bits = []
    bit = 4
    while bit < count:
        bits.append(bit)
        bit *= 2
    spread, last = bits[:-1], bits[-1]
    k_half, c_half = pot_count // 2, cond_count // 2
    c_part = c_half // CHUNKS
    parts = range(CHUNKS)

    blocks = pl.pallas_call(
        functools.partial(prepare_kernel, CHUNKS),
        out_shape=[jax.ShapeDtypeStruct((rows, c_part), BF16)] * (2 * CHUNKS),
        in_specs=[pl.BlockSpec(memory_space=pltpu.SMEM), pl.BlockSpec(memory_space=pltpu.VMEM)],
        out_specs=[pl.BlockSpec(memory_space=pltpu.VMEM)] * (2 * CHUNKS),
        compiler_params=pltpu.CompilerParams(vmem_limit_bytes=6 * 2**20),
        cost_estimate=pl.CostEstimate(flops=10**6, bytes_accessed=2**21, transcendentals=0),
    )(side[None], conduction)
    vals, pots = [valence.T], [potentials.T]
    val_side, pot_side = swap(vals[0], 2), swap(pots[0], 2)
    cond_side = [swap(blocks[part], 2) for part in parts]
    cond_mine = blocks[CHUNKS:]
    vals += [swap(vals[0], 1), val_side, swap(val_side, 1)]
    pots += [swap(pots[0], 1), pot_side, swap(pot_side, 1)]
    cond_core = [swap(cond_mine[part], 1) for part in parts]
    cond_diag = [swap(cond_side[part], 1) for part in parts]
    eig_core = swap(eigenpotentials, 1)
    cond_all = [cond_mine, cond_core, cond_side, cond_diag]

    energies = lax.dynamic_slice(conduction_energy, (side * c_half,), (c_half,))
    factors = (4.0 / points_total) / (valence_energy[:, None] - energies[None, :])

    first, size = core * k_half, k_half
    groups = []
    for bit in spread:
        size //= 2
        up = (me & bit) // bit
        groups.append((first + (1 - up) * size, size))
        first = first + up * size
    groups.append((first, size))

    def pairs_for(place, group):
        block = pots[place]
        return pairs_of(lax.dynamic_slice(block, (group[0], 0), (group[1], block.shape[1])), vals[place])

    starts = jnp.stack([group[0] for group in groups])
    own = [cond_all[place][part] for place in (0, 1) for part in parts]
    own_terms = pl.pallas_call(
        functools.partial(own_kernel, CHUNKS),
        out_shape=[
            jax.ShapeDtypeStruct((group[1] * val_count, c_part), F32) for group in groups for part in parts
        ],
        in_specs=[pl.BlockSpec(memory_space=pltpu.SMEM)] + [pl.BlockSpec(memory_space=pltpu.VMEM)] * (4 + len(own)),
        out_specs=[pl.BlockSpec(memory_space=pltpu.VMEM)] * (len(groups) * CHUNKS),
        scratch_shapes=[
            pltpu.VMEM((groups[0][1] * val_count, 2 * rows), BF16),
            pltpu.VMEM((2 * rows, c_half), BF16),
            pltpu.VMEM((2, pot_count, rows), F32),
        ],
        compiler_params=pltpu.CompilerParams(vmem_limit_bytes=16 * 2**20),
        cost_estimate=pl.CostEstimate(
            flops=4 * rows * k_half * val_count * c_half, bytes_accessed=2**22, transcendentals=0
        ),
    )(starts, vals[0], vals[1], pots[0], pots[1], *own)
    pairs = {place: [pairs_for(place, group) for group in groups] for place in (2, 3)}

    def coefficients(index, part):
        total = own_terms[index * CHUNKS + part]
        for place in (2, 3):
            total = total + contract(pairs[place][index], cond_all[place][part])
        return total

    def cut(block):
        return jnp.split(block, PIECES, axis=0)

    scaled_own = [[None] * CHUNKS for _ in range(PIECES)]
    scaled_rest = [[None] * CHUNKS for _ in range(PIECES)]
    for part in parts:
        totals = [None] * PIECES
        for level, bit in enumerate(spread):
            mine = cut(coefficients(level, part))
            up = (me & bit) // bit
            for q in range(PIECES):
                send, many = mine[q], mine[q].shape[0]
                if totals[q] is not None:
                    totals[q] = totals[q].astype(F32)
                    send = send + lax.dynamic_slice(totals[q], ((1 - up) * many, 0), send.shape)
                    totals[q] = lax.dynamic_slice(totals[q], (up * many, 0), send.shape)
                got = swap(send.astype(BF16), bit)
                totals[q] = got if totals[q] is None else totals[q] + got.astype(F32)
        mine = coefficients(len(spread), part)
        factor = factors[:, part * c_part : (part + 1) * c_part]
        for q in range(PIECES):
            total, low = added(mine, totals[q], q)
            scaled = rescaled(total, swap(low, last), factor)
            scaled_own[q][part] = scaled
            others = []
            for level in reversed(range(len(spread))):
                known = jnp.concatenate([scaled] + others, axis=0)
                others.append(swap(known, spread[level]))
            if others:
                scaled_rest[q][part] = jnp.concatenate(others, axis=0)

    many = k_half // PIECES >> len(spread)

    cond_turned = turned([column for column in cond_all])
    eig_turned = turned([[eigenpotentials], [eig_core]])

    def respond(columns, places):
        blocks = [block for column in columns for block in column]
        height = sum(column[0].shape[0] for column in columns)
        operands = [*blocks, cond_turned, *[vals[place] for place in places]]
        kernel = functools.partial(respond_kernel, places, CHUNKS)
        shape = jax.ShapeDtypeStruct((height // val_count, rows * len(places)), F32)
        return in_vmem(kernel, shape, operands, 10**9, 8, [pltpu.VMEM((height, c_half), BF16)])

    here, there = (0, 1), (2, 3)
    sums = []
    for columns in (scaled_own, scaled_rest):
        if columns[0][0] is not None:
            arrived = swap(respond(columns, there), 2)
            total = respond(columns, here) + arrived
            sums.append(total.reshape(PIECES, -1, many, total.shape[1]))
    width = sums[0].shape[-1]
    response = jnp.concatenate(sums, axis=1).swapaxes(0, 1).reshape(k_half, width)
    for level, bit in enumerate(spread):
        shaped = response.reshape(1 << level, 2, -1, width)
        response = jnp.where((me & bit) != 0, shaped[:, ::-1], shaped).reshape(k_half, width)

    intersection = intersect(response, eig_turned)
    for bit in [2] + spread:
        intersection = intersection + swap(intersection, bit)
    intersection = intersection + swap(intersection.astype(BF16), last).astype(F32)
    squares = jnp.mean(intersection * intersection, axis=1, keepdims=True)
    unit = intersection / jnp.sqrt(squares + 1e-06)
    eig_rows = eig_count // count

    def e_block(device):
        return lax.dynamic_slice(unit, (0, device * eig_rows), (k_half, eig_rows))

    def joined(mine, other):
        return jnp.where(core == 0, jnp.concatenate([mine, other], 0), jnp.concatenate([other, mine], 0))

    projected = finish(core, e_block(me), swap(e_block(me ^ 1), 1))
    remainder, share = outside(response, intersection, [eigenpotentials, eig_core])
    remainder_other = swap(remainder[:, rows:], 1)
    share = share[:, :1].reshape(1, k_half)
    for low_bit, high_bit in zip(bits[::2], bits[1::2] + [0] * (len(bits) % 2)):
        steps = dict.fromkeys(step for step in (low_bit, high_bit, low_bit | high_bit) if step)
        share = share + sum(swap(share, step) for step in steps)
    mine, other = share + swap(share, 2), swap(share, 1) + swap(share, 3)
    sums = joined(mine, other).reshape(pot_count)
    scale = jnp.sqrt(sums / points_total + 1e-06)
    final = lax.optimization_barrier(joined(remainder[:, :rows], remainder_other).T)
    return (projected, final / scale[None, :])


def prepare_kernel(chunks, side_ref, cond_ref, *blocks):
    width = blocks[0].shape[1]
    side = side_ref[0]
    for index, block in enumerate(blocks):
        which = 1 - side if index < chunks else side
        begin = pl.multiple_of((which * chunks + index % chunks) * width, width)
        block[...] = cond_ref[:, pl.ds(begin, width)]


def own_kernel(chunks, starts_ref, val0, val1, pot0, pot1, *refs):
    conds, outs = refs[: 2 * chunks], refs[2 * chunks : -3]
    pairs, right, wide = refs[-3:]
    val_count, rows = val0.shape
    width = conds[0].shape[1]
    for place, (val, pot) in enumerate(((val0, pot0), (val1, pot1))):
        for part in range(chunks):
            right[pl.ds(place * rows, rows), pl.ds(part * width, width)] = conds[place * chunks + part][...]
        wide[place] = pot[...].astype(F32)
    for group in range(len(outs) // chunks):
        height = outs[group * chunks].shape[0]
        many = height // val_count
        start = starts_ref[group]
        for place, val in enumerate((val0, val1)):
            values = val[...].astype(F32)
            for k in range(many):
                row = wide[place, pl.ds(start + k, 1), :]
                pairs[pl.ds(k * val_count, val_count), pl.ds(place * rows, rows)] = (row * values).astype(BF16)
        total = contract(pairs[pl.ds(0, height), :], right[...])
        for part in range(chunks):
            outs[group * chunks + part][...] = total[:, part * width : (part + 1) * width]


def in_vmem(kernel, out_shape, operands, flops, megabytes, scratch=()):
    return pl.pallas_call(
        kernel,
        out_shape=out_shape,
        in_specs=[pl.BlockSpec(memory_space=pltpu.VMEM)] * len(operands),
        out_specs=jax.tree.map(lambda _: pl.BlockSpec(memory_space=pltpu.VMEM), out_shape),
        scratch_shapes=list(scratch),
        compiler_params=pltpu.CompilerParams(vmem_limit_bytes=megabytes * 2**20),
        cost_estimate=pl.CostEstimate(flops=flops, bytes_accessed=2**22, transcendentals=0),
    )(*operands)


def added(block, other, q):
    height = block.shape[0] // PIECES

    def kernel(block_ref, *refs):
        total = block_ref[pl.ds(q * height, height), :]
        for ref in refs[:-2]:
            total = total + ref[...].astype(F32)
        refs[-2][...] = total
        refs[-1][...] = total.astype(BF16)

    shapes = tuple(jax.ShapeDtypeStruct((height, block.shape[1]), kind) for kind in (F32, BF16))
    operands = [block] if other is None else [block, other]
    return in_vmem(kernel, shapes, operands, 10**6, 4)


def rescaled(total, other, factor):
    val_count = factor.shape[0]

    def kernel(total_ref, other_ref, factor_ref, out_ref):
        shaped = (total_ref[...] + other_ref[...].astype(F32)).reshape(-1, val_count, total_ref.shape[1])
        out_ref[...] = (shaped * factor_ref[...][None]).reshape(total_ref.shape).astype(BF16)

    shape = jax.ShapeDtypeStruct(total.shape, BF16)
    return in_vmem(kernel, shape, [total, other, factor], 10**6, 4)


def turned(columns):
    rows = columns[0][0].shape[0]
    depth = sum(block.shape[1] for block in columns[0])
    blocks = [block for column in columns for block in column]

    def kernel(*refs):
        for index, ref in enumerate(refs[:-1]):
            column, part = divmod(index, len(columns[0]))
            size = ref.shape[1]
            refs[-1][part * size : (part + 1) * size, column * rows : (column + 1) * rows] = ref[...].T

    shape = jax.ShapeDtypeStruct((depth, rows * len(columns)), BF16)
    return in_vmem(kernel, shape, blocks, 2 * 10**9, 12)


def finish(core, mine, other):
    def kernel(core_ref, mine_ref, other_ref, out_ref):
        mine, other = mine_ref[...], other_ref[...]
        first = core_ref[0] == 0
        out_ref[...] = jnp.concatenate([jnp.where(first, mine, other), jnp.where(first, other, mine)], axis=0).T

    return pl.pallas_call(
        kernel,
        out_shape=jax.ShapeDtypeStruct((mine.shape[1], 2 * mine.shape[0]), F32),
        in_specs=[pl.BlockSpec(memory_space=pltpu.SMEM)] + [pl.BlockSpec(memory_space=pltpu.VMEM)] * 2,
        out_specs=pl.BlockSpec(memory_space=pltpu.VMEM),
        compiler_params=pltpu.CompilerParams(vmem_limit_bytes=2**21),
        cost_estimate=pl.CostEstimate(flops=10**8, bytes_accessed=2**16, transcendentals=0),
    )(core[None], mine, other)


def intersect(response, eig_turned):
    def kernel(response_ref, eig_ref, out_ref):
        out_ref[...] = contract_last(eig_ref[...], response_ref[...].astype(BF16)).T

    shape = jax.ShapeDtypeStruct((response.shape[0], eig_turned.shape[0]), F32)
    return in_vmem(kernel, shape, [response, eig_turned], 10**9, 8)


def outside(response, intersection, eig_blocks):
    rows = eig_blocks[0].shape[0]

    def kernel(response_ref, part_ref, *refs):
        eigs, (out_ref, share_ref) = refs[:-2], refs[-2:]
        low = part_ref[...].astype(BF16)
        share = jnp.zeros((low.shape[0], 1), F32)
        for index, eig in enumerate(eigs):
            spot = slice(index * rows, (index + 1) * rows)
            left = response_ref[:, spot] - contract_last(eig[...], low).T
            out_ref[:, spot] = left
            share = share + jnp.sum(left * left, axis=1, keepdims=True)
        share_ref[...] = jnp.broadcast_to(share, share_ref.shape)

    shapes = (
        jax.ShapeDtypeStruct(response.shape, F32),
        jax.ShapeDtypeStruct((response.shape[0], 128), F32),
    )
    return in_vmem(kernel, shapes, [response, intersection, *eig_blocks], 10**9, 12)


def respond_kernel(places, chunks, *refs):
    vals = refs[-2 - len(places) : -2]
    right, scaled = refs[-3 - len(places)], refs[: -3 - len(places)]
    out, left = refs[-2:]
    height, depth = left.shape
    width = depth // chunks
    piece = height // (len(scaled) // chunks)
    for index, block in enumerate(scaled):
        q, part = divmod(index, chunks)
        left[pl.ds(q * piece, piece), pl.ds(part * width, width)] = block[...]
    count = out.shape[0]
    val_count = height // count
    rows = out.shape[1] // len(places)
    tile = min(rows, 256)
    for index, place in enumerate(places):

        def step(number, carry):
            begin = pl.multiple_of(number * tile, tile)
            values = vals[index][:, pl.ds(begin, tile)].astype(F32)
            product = contract(left[...], right[:, pl.ds(pl.multiple_of(place * rows + begin, tile), tile)])
            summed = jnp.sum(product.reshape(count, val_count, tile) * values[None], axis=1)
            out[:, pl.ds(pl.multiple_of(index * rows + begin, tile), tile)] = summed
            return carry

        lax.fori_loop(0, rows // tile, step, 0)


def solution(mesh):
    spec = P(("grp", "grid"), None)

    return jax.shard_map(
        body,
        mesh=mesh,
        in_specs=(spec, spec, spec, spec, P("grp"), P("grp")),
        out_specs=(spec, spec),
        check_vma=False,
    )
```

```python
import functools

import jax
import jax.numpy as jnp
from jax import lax
from jax.experimental import pallas as pl
from jax.experimental.pallas import tpu as pltpu

from jax.sharding import PartitionSpec as P

F32 = jnp.float32
BF16 = jnp.bfloat16
CHUNKS = 2
PIECES = 2


def swap(block, bit):
    count = lax.axis_size("grid")
    return lax.ppermute(block, "grid", [(i, i ^ bit) for i in range(count)])


def pairs_of(pot_rows, val_rows):
    joined = pot_rows[:, None, :] * val_rows[None, :, :]
    return joined.reshape(-1, joined.shape[2])


def contract(left, right):
    return jnp.dot(left, right, preferred_element_type=F32)


def contract_last(left, right):
    return lax.dot_general(left, right, (((1,), (1,)), ((), ())), preferred_element_type=F32)


def body(valence, conduction, potentials, eigenpotentials, valence_energy, conduction_energy):
    rows, val_count = valence.shape
    cond_count = conduction.shape[1]
    pot_count = potentials.shape[1]
    eig_count = eigenpotentials.shape[1]
    count = lax.axis_size("grid")
    points_total = rows * count
    me = lax.axis_index("grid")
    core = me & 1
    side = (me >> 1) & 1
    bits = []
    bit = 4
    while bit < count:
        bits.append(bit)
        bit *= 2
    spread, last = bits[:-1], bits[-1]
    k_half, c_half = pot_count // 2, cond_count // 2
    c_part = c_half // CHUNKS
    parts = range(CHUNKS)

    blocks = pl.pallas_call(
        functools.partial(prepare_kernel, CHUNKS),
        out_shape=[jax.ShapeDtypeStruct((rows, c_part), BF16)] * (2 * CHUNKS),
        in_specs=[pl.BlockSpec(memory_space=pltpu.SMEM), pl.BlockSpec(memory_space=pltpu.VMEM)],
        out_specs=[pl.BlockSpec(memory_space=pltpu.VMEM)] * (2 * CHUNKS),
        compiler_params=pltpu.CompilerParams(vmem_limit_bytes=6 * 2**20),
        cost_estimate=pl.CostEstimate(flops=10**6, bytes_accessed=2**21, transcendentals=0),
    )(side[None], conduction)
    vals, pots = [valence.T], [potentials.T]
    val_side, pot_side = swap(vals[0], 2), swap(pots[0], 2)
    cond_side = [swap(blocks[part], 2) for part in parts]
    cond_mine = blocks[CHUNKS:]
    vals += [swap(vals[0], 1), val_side, swap(val_side, 1)]
    pots += [swap(pots[0], 1), pot_side, swap(pot_side, 1)]
    cond_core = [swap(cond_mine[part], 1) for part in parts]
    cond_diag = [swap(cond_side[part], 1) for part in parts]
    eig_core = swap(eigenpotentials, 1)
    cond_all = [cond_mine, cond_core, cond_side, cond_diag]

    energies = lax.dynamic_slice(conduction_energy, (side * c_half,), (c_half,))
    factors = (4.0 / points_total) / (valence_energy[:, None] - energies[None, :])

    first, size = core * k_half, k_half
    groups = []
    for bit in spread:
        size //= 2
        up = (me & bit) // bit
        groups.append((first + (1 - up) * size, size))
        first = first + up * size
    groups.append((first, size))

    def pairs_for(place, group):
        block = pots[place]
        return pairs_of(lax.dynamic_slice(block, (group[0], 0), (group[1], block.shape[1])), vals[place])

    mask = sum((me & bit) // bit << (len(spread) - 1 - level) for level, bit in enumerate(spread))
    marks = jnp.stack([jnp.int32(core), jnp.int32(mask), jnp.int32(me >> 1)] + [group[0] for group in groups])
    own = [cond_all[place][part] for place in (0, 1) for part in parts]
    own_terms = pl.pallas_call(
        functools.partial(own_kernel, CHUNKS),
        out_shape=[
            jax.ShapeDtypeStruct((group[1] * val_count, c_part), F32) for group in groups for part in parts
        ],
        in_specs=[pl.BlockSpec(memory_space=pltpu.SMEM)] + [pl.BlockSpec(memory_space=pltpu.VMEM)] * (4 + len(own)),
        out_specs=[pl.BlockSpec(memory_space=pltpu.VMEM)] * (len(groups) * CHUNKS),
        scratch_shapes=[
            pltpu.VMEM((groups[0][1] * val_count, 2 * rows), BF16),
            pltpu.VMEM((2 * rows, c_half), BF16),
            pltpu.VMEM((2, pot_count, rows), F32),
        ],
        compiler_params=pltpu.CompilerParams(vmem_limit_bytes=16 * 2**20),
        cost_estimate=pl.CostEstimate(
            flops=4 * rows * k_half * val_count * c_half, bytes_accessed=2**22, transcendentals=0
        ),
    )(marks, vals[0], vals[1], pots[0], pots[1], *own)
    pairs = {place: [pairs_for(place, group) for group in groups] for place in (2, 3)}

    def coefficients(index, part):
        total = own_terms[index * CHUNKS + part]
        for place in (2, 3):
            total = total + contract(pairs[place][index], cond_all[place][part])
        return total

    def cut(block):
        return jnp.split(block, PIECES, axis=0)

    scaled_own = [[None] * CHUNKS for _ in range(PIECES)]
    scaled_rest = [[None] * CHUNKS for _ in range(PIECES)]
    for part in parts:
        totals = [None] * PIECES
        for level, bit in enumerate(spread):
            mine = cut(coefficients(level, part))
            up = (me & bit) // bit
            for q in range(PIECES):
                send, many = mine[q], mine[q].shape[0]
                if totals[q] is not None:
                    totals[q] = totals[q].astype(F32)
                    send = send + lax.dynamic_slice(totals[q], ((1 - up) * many, 0), send.shape)
                    totals[q] = lax.dynamic_slice(totals[q], (up * many, 0), send.shape)
                got = swap(send.astype(BF16), bit)
                totals[q] = got if totals[q] is None else totals[q] + got.astype(F32)
        mine = coefficients(len(spread), part)
        factor = factors[:, part * c_part : (part + 1) * c_part]
        for q in range(PIECES):
            total, low = added(mine, totals[q], q)
            scaled = rescaled(total, swap(low, last), factor)
            scaled_own[q][part] = scaled
            others = []
            for level in reversed(range(len(spread))):
                known = jnp.concatenate([scaled] + others, axis=0)
                others.append(swap(known, spread[level]))
            if others:
                scaled_rest[q][part] = jnp.concatenate(others, axis=0)

    many = k_half // PIECES >> len(spread)

    cond_turned = turned([column for column in cond_all])
    eig_turned = [turned([[eigenpotentials]]), turned([[eig_core]])]

    def respond(columns, places):
        blocks = [block for column in columns for block in column]
        height = sum(column[0].shape[0] for column in columns)
        operands = [*blocks, cond_turned, *[vals[place] for place in places]]
        kernel = functools.partial(respond_kernel, places, CHUNKS)
        shape = jax.ShapeDtypeStruct((height // val_count, rows * len(places)), F32)
        return in_vmem(kernel, shape, operands, 10**9, 8, [pltpu.VMEM((height, c_half), BF16)])

    here, there = (0, 1), (2, 3)
    halves = []
    for columns in (scaled_own, scaled_rest):
        if columns[0][0] is not None:
            arrived = swap(respond(columns, there), 2)
            halves.append((respond(columns, here), arrived))

    if many % 8:
        sums = [(near + arrived).reshape(PIECES, -1, many, near.shape[1]) for near, arrived in halves]
        width = sums[0].shape[-1]
        response = jnp.concatenate(sums, axis=1).swapaxes(0, 1).reshape(k_half, width)
        for level, bit in enumerate(spread):
            shaped = response.reshape(1 << level, 2, -1, width)
            response = jnp.where((me & bit) != 0, shaped[:, ::-1], shaped).reshape(k_half, width)
        halves, marks_used = [(response, jnp.zeros_like(response))], jnp.zeros_like(marks)
        response, intersection = intersect(marks_used, halves, eig_turned, k_half)
    else:
        response, intersection = intersect(marks, halves, eig_turned, many)
    for bit in [2] + spread:
        intersection = intersection + swap(intersection, bit)
    intersection = intersection + swap(intersection.astype(BF16), last).astype(F32)
    eig_rows = eig_count // count
    remainder, remainder_core, share, *blocks = outside(
        marks, response, intersection, [eigenpotentials, eig_core], eig_rows
    )
    remainder_other = swap(remainder_core, 1)
    if blocks:
        mine, other = blocks
    else:
        unit = intersection / jnp.sqrt(jnp.mean(intersection * intersection, axis=1, keepdims=True) + 1e-06)
        mine, other = [lax.dynamic_slice(unit, (0, at * eig_rows), (k_half, eig_rows)) for at in (me, me ^ 1)]
    projected = finish(marks, mine, swap(other, 1))
    for low_bit, high_bit in zip(bits[::2], bits[1::2] + [0] * (len(bits) % 2)):
        steps = dict.fromkeys(step for step in (low_bit, high_bit, low_bit | high_bit) if step)
        share = share + sum(swap(share, step) for step in steps)
    mine, other = share + swap(share, 2), swap(share, 1) + swap(share, 3)
    complementary = normalised(marks, mine, other, remainder, remainder_other, points_total)
    return (projected, complementary.T)


def prepare_kernel(chunks, side_ref, cond_ref, *blocks):
    width = blocks[0].shape[1]
    side = side_ref[0]
    for index, block in enumerate(blocks):
        which = 1 - side if index < chunks else side
        begin = pl.multiple_of((which * chunks + index % chunks) * width, width)
        block[...] = cond_ref[:, pl.ds(begin, width)]


def own_kernel(chunks, marks_ref, val0, val1, pot0, pot1, *refs):
    conds, outs = refs[: 2 * chunks], refs[2 * chunks : -3]
    pairs, right, wide = refs[-3:]
    val_count, rows = val0.shape
    width = conds[0].shape[1]
    for place, (val, pot) in enumerate(((val0, pot0), (val1, pot1))):
        for part in range(chunks):
            right[pl.ds(place * rows, rows), pl.ds(part * width, width)] = conds[place * chunks + part][...]
        wide[place] = pot[...].astype(F32)
    for group in range(len(outs) // chunks):
        height = outs[group * chunks].shape[0]
        many = height // val_count
        start = marks_ref[3 + group]
        for place, val in enumerate((val0, val1)):
            values = val[...].astype(F32)
            for k in range(many):
                row = wide[place, pl.ds(start + k, 1), :]
                pairs[pl.ds(k * val_count, val_count), pl.ds(place * rows, rows)] = (row * values).astype(BF16)
        total = contract(pairs[pl.ds(0, height), :], right[...])
        for part in range(chunks):
            outs[group * chunks + part][...] = total[:, part * width : (part + 1) * width]


def in_vmem(kernel, out_shape, operands, flops, megabytes, scratch=()):
    return pl.pallas_call(
        kernel,
        out_shape=out_shape,
        in_specs=[pl.BlockSpec(memory_space=pltpu.VMEM)] * len(operands),
        out_specs=jax.tree.map(lambda _: pl.BlockSpec(memory_space=pltpu.VMEM), out_shape),
        scratch_shapes=list(scratch),
        compiler_params=pltpu.CompilerParams(vmem_limit_bytes=megabytes * 2**20),
        cost_estimate=pl.CostEstimate(flops=flops, bytes_accessed=2**22, transcendentals=0),
    )(*operands)


def added(block, other, q):
    height = block.shape[0] // PIECES

    def kernel(block_ref, *refs):
        total = block_ref[pl.ds(q * height, height), :]
        for ref in refs[:-2]:
            total = total + ref[...].astype(F32)
        refs[-2][...] = total
        refs[-1][...] = total.astype(BF16)

    shapes = tuple(jax.ShapeDtypeStruct((height, block.shape[1]), kind) for kind in (F32, BF16))
    operands = [block] if other is None else [block, other]
    return in_vmem(kernel, shapes, operands, 10**6, 4)


def rescaled(total, other, factor):
    val_count = factor.shape[0]

    def kernel(total_ref, other_ref, factor_ref, out_ref):
        shaped = (total_ref[...] + other_ref[...].astype(F32)).reshape(-1, val_count, total_ref.shape[1])
        out_ref[...] = (shaped * factor_ref[...][None]).reshape(total_ref.shape).astype(BF16)

    shape = jax.ShapeDtypeStruct(total.shape, BF16)
    return in_vmem(kernel, shape, [total, other, factor], 10**6, 4)


def turned(columns):
    rows = columns[0][0].shape[0]
    depth = sum(block.shape[1] for block in columns[0])
    blocks = [block for column in columns for block in column]

    def kernel(*refs):
        for index, ref in enumerate(refs[:-1]):
            column, part = divmod(index, len(columns[0]))
            size = ref.shape[1]
            refs[-1][part * size : (part + 1) * size, column * rows : (column + 1) * rows] = ref[...].T

    shape = jax.ShapeDtypeStruct((depth, rows * len(columns)), BF16)
    return in_vmem(kernel, shape, blocks, 2 * 10**9, 12)


def with_marks(kernel, out_shape, operands, megabytes):
    return pl.pallas_call(
        kernel,
        out_shape=out_shape,
        in_specs=[pl.BlockSpec(memory_space=pltpu.SMEM)]
        + [pl.BlockSpec(memory_space=pltpu.VMEM)] * (len(operands) - 1),
        out_specs=jax.tree.map(lambda _: pl.BlockSpec(memory_space=pltpu.VMEM), out_shape),
        compiler_params=pltpu.CompilerParams(vmem_limit_bytes=megabytes * 2**20),
        cost_estimate=pl.CostEstimate(flops=10**9, bytes_accessed=2**22, transcendentals=0),
    )(*operands)


def finish(marks, mine, other):
    def kernel(marks_ref, mine_ref, other_ref, out_ref):
        mine, other = mine_ref[...], other_ref[...]
        first = marks_ref[0] == 0
        out_ref[...] = jnp.concatenate([jnp.where(first, mine, other), jnp.where(first, other, mine)], axis=0).T

    shape = jax.ShapeDtypeStruct((mine.shape[1], 2 * mine.shape[0]), F32)
    return with_marks(kernel, shape, [marks, mine, other], 2)


def intersect(marks, halves, eig_turned, many):
    rows = eig_turned[0].shape[1]
    width = halves[0][0].shape[1]
    height = sum(near.shape[0] for near, _ in halves)
    own = halves[0][0].shape[0] // many
    blocks = height // (own * many)

    def kernel(marks_ref, *refs):
        eigs, (response_ref, out_ref) = refs[-2 - len(eig_turned) : -2], refs[-2:]
        mask = marks_ref[1]
        for q in range(own):
            for block in range(blocks):
                near, arrived = refs[0:2] if block == 0 else refs[2:4]
                top = q * many if block == 0 else (q * (blocks - 1) + block - 1) * many
                spot = (block ^ mask) * (own * many) + q * many
                spot = pl.ds(pl.multiple_of(spot, many), many)
                response_ref[spot, :] = near[top : top + many, :] + arrived[top : top + many, :]
        total = None
        for index, eig in enumerate(eigs):
            low = response_ref[:, index * rows : (index + 1) * rows].astype(BF16)
            term = contract_last(eig[...], low)
            total = term if total is None else total + term
        out_ref[...] = total.T

    shapes = (
        jax.ShapeDtypeStruct((height, width), F32),
        jax.ShapeDtypeStruct((height, eig_turned[0].shape[0]), F32),
    )
    operands = [marks, *[block for pair in halves for block in pair], *eig_turned]
    return with_marks(kernel, shapes, operands, 8)


def outside(marks, response, intersection, eig_blocks, eig_rows):
    rows, eig_count = eig_blocks[0].shape
    count = response.shape[0]
    pair = 2 * eig_rows

    def kernel(marks_ref, response_ref, part_ref, *refs):
        eigs, outs = refs[: len(eig_blocks)], refs[len(eig_blocks) :]
        low = part_ref[...].astype(BF16)
        share = jnp.zeros((count, 1), F32)
        for index, eig in enumerate(eigs):
            spot = slice(index * rows, (index + 1) * rows)
            left = response_ref[:, spot] - contract_last(eig[...], low).T
            outs[index][...] = left
            share = share + jnp.sum(left * left, axis=1, keepdims=True)
        outs[2][...] = jnp.sum(jnp.where(diagonal(count), share, 0.0), axis=0, keepdims=True)
        if len(outs) > 3:
            squares = jnp.sum(part_ref[...] * part_ref[...], axis=1, keepdims=True) / eig_count
            window = part_ref[:, pl.ds(pl.multiple_of(marks_ref[2] * pair, pair), pair)]
            window = window / jnp.sqrt(squares + 1e-06)
            first = marks_ref[0] == 0
            outs[3][...] = jnp.where(first, window[:, :eig_rows], window[:, eig_rows:])
            outs[4][...] = jnp.where(first, window[:, eig_rows:], window[:, :eig_rows])

    sizes = [(count, rows), (count, rows), (1, count)] + ([] if pair % 128 else [(count, eig_rows)] * 2)
    shapes = tuple(jax.ShapeDtypeStruct(size, F32) for size in sizes)
    return with_marks(kernel, shapes, [marks, response, intersection, *eig_blocks], 12)


def diagonal(size):
    shape = (size, size)
    return lax.broadcasted_iota(jnp.int32, shape, 0) == lax.broadcasted_iota(jnp.int32, shape, 1)


def normalised(marks, sum_mine, sum_other, mine, other, points_total):
    height, width = mine.shape

    def kernel(marks_ref, sum_mine_ref, sum_other_ref, mine_ref, other_ref, out_ref):
        core = marks_ref[0]
        for row_ref, block_ref, half in ((sum_mine_ref, mine_ref, core), (sum_other_ref, other_ref, 1 - core)):
            column = jnp.sum(jnp.where(diagonal(height), row_ref[...], 0.0), axis=1, keepdims=True)
            block = block_ref[...] / jnp.sqrt(column / points_total + 1e-06)
            out_ref[pl.ds(pl.multiple_of(half * height, height), height), :] = block

    shape = jax.ShapeDtypeStruct((2 * height, width), F32)
    return with_marks(kernel, shape, [marks, sum_mine, sum_other, mine, other], 4)


def respond_kernel(places, chunks, *refs):
    vals = refs[-2 - len(places) : -2]
    right, scaled = refs[-3 - len(places)], refs[: -3 - len(places)]
    out, left = refs[-2:]
    height, depth = left.shape
    width = depth // chunks
    piece = height // (len(scaled) // chunks)
    for index, block in enumerate(scaled):
        q, part = divmod(index, chunks)
        left[pl.ds(q * piece, piece), pl.ds(part * width, width)] = block[...]
    count = out.shape[0]
    val_count = height // count
    rows = out.shape[1] // len(places)
    tile = min(rows, 256)
    for index, place in enumerate(places):

        def step(number, carry):
            begin = pl.multiple_of(number * tile, tile)
            values = vals[index][:, pl.ds(begin, tile)].astype(F32)
            product = contract(left[...], right[:, pl.ds(pl.multiple_of(place * rows + begin, tile), tile)])
            summed = jnp.sum(product.reshape(count, val_count, tile) * values[None], axis=1)
            out[:, pl.ds(pl.multiple_of(index * rows + begin, tile), tile)] = summed
            return carry

        lax.fori_loop(0, rows // tile, step, 0)


def solution(mesh):
    spec = P(("grp", "grid"), None)

    return jax.shard_map(
        body,
        mesh=mesh,
        in_specs=(spec, spec, spec, spec, P("grp"), P("grp")),
        out_specs=(spec, spec),
        check_vma=False,
    )
```

```python
import functools

import jax
import jax.numpy as jnp
from jax import lax
from jax.experimental import pallas as pl
from jax.experimental.pallas import tpu as pltpu

from jax.sharding import PartitionSpec as P

F32 = jnp.float32
BF16 = jnp.bfloat16
CHUNKS = 2
PIECES = 2


def swap(block, bit):
    count = lax.axis_size("grid")
    return lax.ppermute(block, "grid", [(i, i ^ bit) for i in range(count)])


def pairs_of(pot_rows, val_rows):
    joined = pot_rows[:, None, :] * val_rows[None, :, :]
    return joined.reshape(-1, joined.shape[2])


def contract(left, right):
    return jnp.dot(left, right, preferred_element_type=F32)


def contract_last(left, right):
    return lax.dot_general(left, right, (((1,), (1,)), ((), ())), preferred_element_type=F32)


def body(valence, conduction, potentials, eigenpotentials, valence_energy, conduction_energy):
    rows, val_count = valence.shape
    cond_count = conduction.shape[1]
    pot_count = potentials.shape[1]
    eig_count = eigenpotentials.shape[1]
    count = lax.axis_size("grid")
    points_total = rows * count
    me = lax.axis_index("grid")
    core = me & 1
    side = (me >> 1) & 1
    bits = []
    bit = 4
    while bit < count:
        bits.append(bit)
        bit *= 2
    spread, last = bits[:-1], bits[-1]
    k_half, c_half = pot_count // 2, cond_count // 2
    c_part = c_half // CHUNKS
    parts = range(CHUNKS)

    blocks = pl.pallas_call(
        functools.partial(prepare_kernel, CHUNKS),
        out_shape=[jax.ShapeDtypeStruct((rows, c_part), BF16)] * (2 * CHUNKS),
        in_specs=[pl.BlockSpec(memory_space=pltpu.SMEM), pl.BlockSpec(memory_space=pltpu.VMEM)],
        out_specs=[pl.BlockSpec(memory_space=pltpu.VMEM)] * (2 * CHUNKS),
        compiler_params=pltpu.CompilerParams(vmem_limit_bytes=6 * 2**20),
        cost_estimate=pl.CostEstimate(flops=10**6, bytes_accessed=2**21, transcendentals=0),
    )(side[None], conduction)
    vals, pots = [valence.T], [potentials.T]
    val_side, pot_side = swap(vals[0], 2), swap(pots[0], 2)
    cond_side = [swap(blocks[part], 2) for part in parts]
    cond_mine = blocks[CHUNKS:]
    vals += [swap(vals[0], 1), val_side, swap(val_side, 1)]
    pots += [swap(pots[0], 1), pot_side, swap(pot_side, 1)]
    cond_core = [swap(cond_mine[part], 1) for part in parts]
    cond_diag = [swap(cond_side[part], 1) for part in parts]
    eig_core = swap(eigenpotentials, 1)
    cond_all = [cond_mine, cond_core, cond_side, cond_diag]

    energies = lax.dynamic_slice(conduction_energy, (side * c_half,), (c_half,))
    factors = (4.0 / points_total) / (valence_energy[:, None] - energies[None, :])

    first, size = core * k_half, k_half
    groups = []
    for bit in spread:
        size //= 2
        up = (me & bit) // bit
        groups.append((first + (1 - up) * size, size))
        first = first + up * size
    groups.append((first, size))

    def pairs_for(place, group):
        block = pots[place]
        return pairs_of(lax.dynamic_slice(block, (group[0], 0), (group[1], block.shape[1])), vals[place])

    mask = sum((me & bit) // bit << (len(spread) - 1 - level) for level, bit in enumerate(spread))
    marks = jnp.stack([jnp.int32(core), jnp.int32(mask), jnp.int32(me >> 1)] + [group[0] for group in groups])
    own = [cond_all[place][part] for place in (0, 1) for part in parts]
    *own_terms, vals[0], vals[1] = pl.pallas_call(
        functools.partial(own_kernel, CHUNKS),
        out_shape=[
            jax.ShapeDtypeStruct((group[1] * val_count, c_part), F32) for group in groups for part in parts
        ]
        + [jax.ShapeDtypeStruct(vals[0].shape, BF16)] * 2,
        in_specs=[pl.BlockSpec(memory_space=pltpu.SMEM)] + [pl.BlockSpec(memory_space=pltpu.VMEM)] * (4 + len(own)),
        out_specs=[pl.BlockSpec(memory_space=pltpu.VMEM)] * (len(groups) * CHUNKS + 2),
        scratch_shapes=[
            pltpu.VMEM((groups[0][1] * val_count, 2 * rows), BF16),
            pltpu.VMEM((2 * rows, c_half), BF16),
            pltpu.VMEM((2, pot_count, rows), F32),
        ],
        compiler_params=pltpu.CompilerParams(vmem_limit_bytes=16 * 2**20),
        cost_estimate=pl.CostEstimate(
            flops=4 * rows * k_half * val_count * c_half, bytes_accessed=2**22, transcendentals=0
        ),
    )(marks, vals[0], vals[1], pots[0], pots[1], *own)
    pairs = {place: [pairs_for(place, group) for group in groups] for place in (2, 3)}

    def coefficients(index, part):
        total = own_terms[index * CHUNKS + part]
        for place in (2, 3):
            total = total + contract(pairs[place][index], cond_all[place][part])
        return total

    def cut(block):
        return jnp.split(block, PIECES, axis=0)

    scaled_own = [[None] * CHUNKS for _ in range(PIECES)]
    scaled_rest = [[None] * CHUNKS for _ in range(PIECES)]
    for part in parts:
        totals = [None] * PIECES
        for level, bit in enumerate(spread):
            mine = cut(coefficients(level, part))
            up = (me & bit) // bit
            for q in range(PIECES):
                send, many = mine[q], mine[q].shape[0]
                if totals[q] is not None:
                    totals[q] = totals[q].astype(F32)
                    send = send + lax.dynamic_slice(totals[q], ((1 - up) * many, 0), send.shape)
                    totals[q] = lax.dynamic_slice(totals[q], (up * many, 0), send.shape)
                got = swap(send.astype(BF16), bit)
                totals[q] = got if totals[q] is None else totals[q] + got.astype(F32)
        mine = coefficients(len(spread), part)
        factor = factors[:, part * c_part : (part + 1) * c_part]
        for q in range(PIECES):
            total, low = added(mine, totals[q], q)
            scaled = rescaled(total, swap(low, last), factor)
            scaled_own[q][part] = scaled
            others = []
            for level in reversed(range(len(spread))):
                known = jnp.concatenate([scaled] + others, axis=0)
                others.append(swap(known, spread[level]))
            if others:
                scaled_rest[q][part] = jnp.concatenate(others, axis=0)

    many = k_half // PIECES >> len(spread)

    cond_turned = turned([column for column in cond_all])
    eig_turned = [turned([[eigenpotentials]]), turned([[eig_core]])]

    def respond(columns, places):
        blocks = [block for column in columns for block in column]
        height = sum(column[0].shape[0] for column in columns)
        operands = [*blocks, cond_turned, *[vals[place] for place in places]]
        kernel = functools.partial(respond_kernel, places, CHUNKS)
        shape = jax.ShapeDtypeStruct((height // val_count, rows * len(places)), F32)
        return in_vmem(kernel, shape, operands, 10**9, 8, [pltpu.VMEM((height, c_half), BF16)])

    here, there = (0, 1), (2, 3)
    halves = []
    for columns in (scaled_own, scaled_rest):
        if columns[0][0] is not None:
            arrived = swap(respond(columns, there), 2)
            halves.append((respond(columns, here), arrived))

    if many % 8:
        sums = [(near + arrived).reshape(PIECES, -1, many, near.shape[1]) for near, arrived in halves]
        width = sums[0].shape[-1]
        response = jnp.concatenate(sums, axis=1).swapaxes(0, 1).reshape(k_half, width)
        for level, bit in enumerate(spread):
            shaped = response.reshape(1 << level, 2, -1, width)
            response = jnp.where((me & bit) != 0, shaped[:, ::-1], shaped).reshape(k_half, width)
        halves, marks_used = [(response, jnp.zeros_like(response))], jnp.zeros_like(marks)
        response, intersection = intersect(marks_used, halves, eig_turned, k_half)
    else:
        response, intersection = intersect(marks, halves, eig_turned, many)
    for bit in [2] + spread:
        intersection = intersection + swap(intersection, bit)
    intersection = intersection + swap(intersection.astype(BF16), last).astype(F32)
    eig_rows = eig_count // count
    remainder, remainder_core, share, *blocks = outside(
        marks, response, intersection, [eigenpotentials, eig_core], eig_rows
    )
    remainder_other = swap(remainder_core, 1)
    if blocks:
        mine, other = blocks
    else:
        unit = intersection / jnp.sqrt(jnp.mean(intersection * intersection, axis=1, keepdims=True) + 1e-06)
        mine, other = [lax.dynamic_slice(unit, (0, at * eig_rows), (k_half, eig_rows)) for at in (me, me ^ 1)]
    projected = finish(marks, mine, swap(other, 1))
    for low_bit, high_bit in zip(bits[::2], bits[1::2] + [0] * (len(bits) % 2)):
        steps = dict.fromkeys(step for step in (low_bit, high_bit, low_bit | high_bit) if step)
        share = share + sum(swap(share, step) for step in steps)
    mine, other = share + swap(share, 2), swap(share, 1) + swap(share, 3)
    complementary = normalised(marks, mine, other, remainder, remainder_other, points_total)
    return (projected, complementary.T)


def prepare_kernel(chunks, side_ref, cond_ref, *blocks):
    width = blocks[0].shape[1]
    side = side_ref[0]
    for index, block in enumerate(blocks):
        which = 1 - side if index < chunks else side
        begin = pl.multiple_of((which * chunks + index % chunks) * width, width)
        block[...] = cond_ref[:, pl.ds(begin, width)]


def own_kernel(chunks, marks_ref, val0, val1, pot0, pot1, *refs):
    conds, outs, kept = refs[: 2 * chunks], refs[2 * chunks : -5], refs[-5:-3]
    kept[0][...], kept[1][...] = val0[...], val1[...]
    pairs, right, wide = refs[-3:]
    val_count, rows = val0.shape
    width = conds[0].shape[1]
    for place, (val, pot) in enumerate(((val0, pot0), (val1, pot1))):
        for part in range(chunks):
            right[pl.ds(place * rows, rows), pl.ds(part * width, width)] = conds[place * chunks + part][...]
        wide[place] = pot[...].astype(F32)
    for group in range(len(outs) // chunks):
        height = outs[group * chunks].shape[0]
        many = height // val_count
        start = marks_ref[3 + group]
        for place, val in enumerate((val0, val1)):
            values = val[...].astype(F32)
            for k in range(many):
                row = wide[place, pl.ds(start + k, 1), :]
                pairs[pl.ds(k * val_count, val_count), pl.ds(place * rows, rows)] = (row * values).astype(BF16)
        total = contract(pairs[pl.ds(0, height), :], right[...])
        for part in range(chunks):
            outs[group * chunks + part][...] = total[:, part * width : (part + 1) * width]


def in_vmem(kernel, out_shape, operands, flops, megabytes, scratch=()):
    return pl.pallas_call(
        kernel,
        out_shape=out_shape,
        in_specs=[pl.BlockSpec(memory_space=pltpu.VMEM)] * len(operands),
        out_specs=jax.tree.map(lambda _: pl.BlockSpec(memory_space=pltpu.VMEM), out_shape),
        scratch_shapes=list(scratch),
        compiler_params=pltpu.CompilerParams(vmem_limit_bytes=megabytes * 2**20),
        cost_estimate=pl.CostEstimate(flops=flops, bytes_accessed=2**22, transcendentals=0),
    )(*operands)


def added(block, other, q):
    height = block.shape[0] // PIECES

    def kernel(block_ref, *refs):
        total = block_ref[pl.ds(q * height, height), :]
        for ref in refs[:-2]:
            total = total + ref[...].astype(F32)
        refs[-2][...] = total
        refs[-1][...] = total.astype(BF16)

    shapes = tuple(jax.ShapeDtypeStruct((height, block.shape[1]), kind) for kind in (F32, BF16))
    operands = [block] if other is None else [block, other]
    return in_vmem(kernel, shapes, operands, 10**6, 4)


def rescaled(total, other, factor):
    val_count = factor.shape[0]

    def kernel(total_ref, other_ref, factor_ref, out_ref):
        shaped = (total_ref[...] + other_ref[...].astype(F32)).reshape(-1, val_count, total_ref.shape[1])
        out_ref[...] = (shaped * factor_ref[...][None]).reshape(total_ref.shape).astype(BF16)

    shape = jax.ShapeDtypeStruct(total.shape, BF16)
    return in_vmem(kernel, shape, [total, other, factor], 10**6, 4)


def turned(columns):
    rows = columns[0][0].shape[0]
    depth = sum(block.shape[1] for block in columns[0])
    blocks = [block for column in columns for block in column]

    def kernel(*refs):
        for index, ref in enumerate(refs[:-1]):
            column, part = divmod(index, len(columns[0]))
            size = ref.shape[1]
            refs[-1][part * size : (part + 1) * size, column * rows : (column + 1) * rows] = ref[...].T

    shape = jax.ShapeDtypeStruct((depth, rows * len(columns)), BF16)
    return in_vmem(kernel, shape, blocks, 2 * 10**9, 12)


def with_marks(kernel, out_shape, operands, megabytes):
    return pl.pallas_call(
        kernel,
        out_shape=out_shape,
        in_specs=[pl.BlockSpec(memory_space=pltpu.SMEM)]
        + [pl.BlockSpec(memory_space=pltpu.VMEM)] * (len(operands) - 1),
        out_specs=jax.tree.map(lambda _: pl.BlockSpec(memory_space=pltpu.VMEM), out_shape),
        compiler_params=pltpu.CompilerParams(vmem_limit_bytes=megabytes * 2**20),
        cost_estimate=pl.CostEstimate(flops=10**9, bytes_accessed=2**22, transcendentals=0),
    )(*operands)


def finish(marks, mine, other):
    def kernel(marks_ref, mine_ref, other_ref, out_ref):
        mine, other = mine_ref[...], other_ref[...]
        first = marks_ref[0] == 0
        out_ref[...] = jnp.concatenate([jnp.where(first, mine, other), jnp.where(first, other, mine)], axis=0).T

    shape = jax.ShapeDtypeStruct((mine.shape[1], 2 * mine.shape[0]), F32)
    return with_marks(kernel, shape, [marks, mine, other], 2)


def intersect(marks, halves, eig_turned, many):
    rows = eig_turned[0].shape[1]
    width = halves[0][0].shape[1]
    height = sum(near.shape[0] for near, _ in halves)
    own = halves[0][0].shape[0] // many
    blocks = height // (own * many)

    def kernel(marks_ref, *refs):
        eigs, (response_ref, out_ref) = refs[-2 - len(eig_turned) : -2], refs[-2:]
        mask = marks_ref[1]
        for q in range(own):
            for block in range(blocks):
                near, arrived = refs[0:2] if block == 0 else refs[2:4]
                top = q * many if block == 0 else (q * (blocks - 1) + block - 1) * many
                spot = (block ^ mask) * (own * many) + q * many
                spot = pl.ds(pl.multiple_of(spot, many), many)
                response_ref[spot, :] = near[top : top + many, :] + arrived[top : top + many, :]
        total = None
        for index, eig in enumerate(eigs):
            low = response_ref[:, index * rows : (index + 1) * rows].astype(BF16)
            term = contract_last(eig[...], low)
            total = term if total is None else total + term
        out_ref[...] = total.T

    shapes = (
        jax.ShapeDtypeStruct((height, width), F32),
        jax.ShapeDtypeStruct((height, eig_turned[0].shape[0]), F32),
    )
    operands = [marks, *[block for pair in halves for block in pair], *eig_turned]
    return with_marks(kernel, shapes, operands, 8)


def outside(marks, response, intersection, eig_blocks, eig_rows):
    rows, eig_count = eig_blocks[0].shape
    count = response.shape[0]
    pair = 2 * eig_rows

    def kernel(marks_ref, response_ref, part_ref, *refs):
        eigs, outs = refs[: len(eig_blocks)], refs[len(eig_blocks) :]
        low = part_ref[...].astype(BF16)
        share = jnp.zeros((count, 1), F32)
        for index, eig in enumerate(eigs):
            spot = slice(index * rows, (index + 1) * rows)
            left = response_ref[:, spot] - contract_last(eig[...], low).T
            outs[index][...] = left
            share = share + jnp.sum(left * left, axis=1, keepdims=True)
        outs[2][...] = jnp.sum(jnp.where(diagonal(count), share, 0.0), axis=0, keepdims=True)
        if len(outs) > 3:
            squares = jnp.sum(part_ref[...] * part_ref[...], axis=1, keepdims=True) / eig_count
            window = part_ref[:, pl.ds(pl.multiple_of(marks_ref[2] * pair, pair), pair)]
            window = window / jnp.sqrt(squares + 1e-06)
            first = marks_ref[0] == 0
            outs[3][...] = jnp.where(first, window[:, :eig_rows], window[:, eig_rows:])
            outs[4][...] = jnp.where(first, window[:, eig_rows:], window[:, :eig_rows])

    sizes = [(count, rows), (count, rows), (1, count)] + ([] if pair % 128 else [(count, eig_rows)] * 2)
    shapes = tuple(jax.ShapeDtypeStruct(size, F32) for size in sizes)
    return with_marks(kernel, shapes, [marks, response, intersection, *eig_blocks], 12)


def diagonal(size):
    shape = (size, size)
    return lax.broadcasted_iota(jnp.int32, shape, 0) == lax.broadcasted_iota(jnp.int32, shape, 1)


def normalised(marks, sum_mine, sum_other, mine, other, points_total):
    height, width = mine.shape

    def kernel(marks_ref, sum_mine_ref, sum_other_ref, mine_ref, other_ref, out_ref):
        core = marks_ref[0]
        for row_ref, block_ref, half in ((sum_mine_ref, mine_ref, core), (sum_other_ref, other_ref, 1 - core)):
            column = jnp.sum(jnp.where(diagonal(height), row_ref[...], 0.0), axis=1, keepdims=True)
            block = block_ref[...] / jnp.sqrt(column / points_total + 1e-06)
            out_ref[pl.ds(pl.multiple_of(half * height, height), height), :] = block

    shape = jax.ShapeDtypeStruct((2 * height, width), F32)
    return with_marks(kernel, shape, [marks, sum_mine, sum_other, mine, other], 4)


def respond_kernel(places, chunks, *refs):
    vals = refs[-2 - len(places) : -2]
    right, scaled = refs[-3 - len(places)], refs[: -3 - len(places)]
    out, left = refs[-2:]
    height, depth = left.shape
    width = depth // chunks
    piece = height // (len(scaled) // chunks)
    for index, block in enumerate(scaled):
        q, part = divmod(index, chunks)
        left[pl.ds(q * piece, piece), pl.ds(part * width, width)] = block[...]
    count = out.shape[0]
    val_count = height // count
    rows = out.shape[1] // len(places)
    tile = min(rows, 256)
    for index, place in enumerate(places):

        def step(number, carry):
            begin = pl.multiple_of(number * tile, tile)
            values = vals[index][:, pl.ds(begin, tile)].astype(F32)
            product = contract(left[...], right[:, pl.ds(pl.multiple_of(place * rows + begin, tile), tile)])
            summed = jnp.sum(product.reshape(count, val_count, tile) * values[None], axis=1)
            out[:, pl.ds(pl.multiple_of(index * rows + begin, tile), tile)] = summed
            return carry

        lax.fori_loop(0, rows // tile, step, 0)


def solution(mesh):
    spec = P(("grp", "grid"), None)

    return jax.shard_map(
        body,
        mesh=mesh,
        in_specs=(spec, spec, spec, spec, P("grp"), P("grp")),
        out_specs=(spec, spec),
        check_vma=False,
    )
```
